32 devices in a mesh: row: 8 (over y, x, core), col: 4 (over z).
Axes of the slice: x: 2, y: 2, z: 4, core: 2. Of those that a mesh axis runs over, the one named last changes fastest.
Arguments:
- a_window: float32 [16384, 4096], P('row', 'col'), may hold values from -6 to 6
- l_panel: float32 [16384, 1024], P('row'), may hold values from -0.1875 to 0.1875
- l_inverse: float32 [2, 512, 512], replicated, may hold values from -2 to 2, as said below
Outputs:
- reduced: float32 [16384, 4096], P('row', 'col')
The draws below stay inside these ranges and needn't reach their ends.
Inputs may be any that keep to these rules, and one draw needn't show every extreme that they name: `l_inverse`: both blocks are lower triangular, with diagonal entries between 0.5 and 2.
All inputs are finite; a program needn't handle non-finite values.
Results may differ from the reference program's by a relative error of at most 0.000067.
Values sent between devices are 32-bit elements; how exact they have to be, the bound alone decides.
A program may use at most 128 MiB of HBM per device.

```python
import jax
import jax.numpy as jnp
from jax import lax

N = 16384
B = 512
WC = 4096


def draw_l_inverse(key, part):
    first_key, second_key = jax.random.split(jax.random.fold_in(key, 17))
    spread = jnp.clip(jax.random.normal(first_key, (2, B, B), jnp.float32), -4.0, 4.0)
    diagonal = jax.random.uniform(second_key, (2, B), jnp.float32, 0.5, 1.5)
    strict = jnp.tril(spread, -1) / jnp.sqrt(jnp.float32(B))
    return strict + diagonal[:, :, None] * jnp.eye(B, dtype=jnp.float32)[None, :, :]


def shard_levels(own_key, extent, pieces, least, top_value):
    level, own = 1.0, jax.random.fold_in(own_key, 6)
    for axis_at, shards_of in pieces:
        steps = jnp.exp(jax.random.uniform(jax.random.fold_in(own, axis_at), (shards_of,), jnp.float32, least / len(pieces), top_value / len(pieces)))
        level = level * jnp.repeat(steps, extent[axis_at] // shards_of).reshape([-1 if axis == axis_at else 1 for axis in range(len(extent))])
    return level


def noise(own_key, shape, deviation, reach, cuts=(), kind=jnp.bfloat16):
    loudness = shard_levels(own_key, shape, cuts, -0.22, 0.18) if cuts else 1.0
    drawn = jax.random.normal(own_key, shape, jnp.float32) * deviation * loudness
    return jnp.minimum(jnp.maximum(drawn, -reach), reach).astype(kind)


def setup_inputs(seed: int = 0) -> dict:
    key_list = jax.random.split(jax.random.key(seed), 4)
    a_window = noise(key_list[0], (N, WC), 1.0, 6.0, ((0, 8), (1, 4)), jnp.float32)
    l_panel = noise(key_list[1], (N, 2 * B), (2 * B) ** -0.5, 0.1875, ((0, 8),), jnp.float32)
    l_inverse = draw_l_inverse(jax.random.fold_in(key_list[3], 71), 0)
    return {"a_window": a_window, "l_panel": l_panel, "l_inverse": l_inverse}


def matmul_hp(left, right):
    return jnp.dot(left, right, precision=lax.Precision.HIGHEST, preferred_element_type=jnp.float32)


def reference(a_window, l_panel, l_inverse):
    first_inv = l_inverse[0]
    second_inv = l_inverse[1]
    coupling = l_panel[B:2 * B, :B]
    leading = matmul_hp(a_window[:, :B], first_inv.T)
    second_col = matmul_hp(a_window[:, B:2 * B] - matmul_hp(leading, coupling.T), second_inv.T)
    solved = jnp.concatenate([leading, second_col], 1)
    upper_tile = matmul_hp(first_inv, solved[:B])
    lower_tile = matmul_hp(second_inv, solved[B:2 * B] - matmul_hp(coupling, upper_tile))
    diag_block = jnp.concatenate([upper_tile, lower_tile], 0)
    below = l_panel[2 * B:]
    product = matmul_hp(below, diag_block)
    reduced_g = solved[2 * B:] - 0.5 * product
    lower_panel = solved[2 * B:] - product
    width_left = WC - 2 * B
    update = a_window[2 * B:, 2 * B:] - matmul_hp(below, reduced_g[:width_left].T) - matmul_hp(reduced_g, below[:width_left].T)
    upper_rows = jnp.concatenate([diag_block, a_window[:2 * B, 2 * B:]], 1)
    lower_rows = jnp.concatenate([lower_panel, update], 1)
    return jnp.concatenate([upper_rows, lower_rows], 0)
```

```python
import functools

import jax
import jax.numpy as jnp
from jax import lax
from jax.experimental import pallas as pl
from jax.experimental.pallas import tpu as pltpu
from jax.sharding import PartitionSpec as P

MESH = pl.DeviceIdType.MESH
SPAN = 16
TILE = 256
AHEAD = 8
LAG = 3
NN, NT = ((1,), (0,)), ((1,), (1,))
COUPLE, LOWER, TOP, TILEROWS = range(4)


def bits_of(count):
    return max(count.bit_length() - 1, 0)


def ring_pos(index, count):
    if count & (count - 1):
        return index
    parity, place = 0, 0
    for bit in reversed(range(bits_of(count))):
        parity = (parity + (index // 2**bit) % 2) % 2
        place = place + parity * 2**bit
    return place


def ring_at(place, count):
    if count & (count - 1):
        return place
    index = 0
    for bit in range(bits_of(count)):
        index = index + (((place // 2**bit) % 2 + (place // 2 ** (bit + 1)) % 2) % 2) * 2**bit
    return index


def seen_from(index, root, count):
    if count & (count - 1):
        return (index - root + count) % count
    return sum((((index // 2**bit) % 2 + (root // 2**bit) % 2) % 2) * 2**bit for bit in range(bits_of(count)))


def placed_from(offset, root, count):
    if count & (count - 1):
        return (offset + root) % count
    return seen_from(offset, root, count)


def split(value):
    high = value.astype(jnp.bfloat16)
    return high, (value - high.astype(jnp.float32)).astype(jnp.bfloat16)


def dot3(left_high, left_low, high, low, dims):
    total = lax.dot_general(left_high, high, (dims, ((), ())), preferred_element_type=jnp.float32)
    total += lax.dot_general(left_high, low, (dims, ((), ())), preferred_element_type=jnp.float32)
    return total + lax.dot_general(left_low, high, (dims, ((), ())), preferred_element_type=jnp.float32)


def full_dot(left, right):
    return lax.dot_general(
        left, right, (NN, ((), ())), precision=lax.Precision.HIGHEST, preferred_element_type=jnp.float32
    )


def step_kernel(
    rows_n, cols_n, a_ref, l_ref, i_ref, out_ref,
    zbuf, top, tile, low, couple, part, work, lh, ll, ih, il, kh, kl, ch, cl, vh, vl,
    zs, zr, cs, cr, ls, lr, ts, tr, gs, gr, here,
):
    row, col = lax.axis_index("row"), lax.axis_index("col")
    depth, width = a_ref.shape
    half = i_ref.shape[1]
    pieces = depth // SPAN
    top_pieces = width // SPAN
    tile_n = min(TILE, width)
    blocks, groups = depth // tile_n, width // tile_n
    per_block = tile_n // SPAN
    small = min(128, half)
    panel = col == 0
    relays = jnp.logical_and(col != 0, col != cols_n - 1)
    root = (col * width) // depth
    offset = (col * width) % depth
    pair = 2 if rows_n % 2 == 0 else 1
    chain = rows_n // pair
    most = chain - 1 + pair - 1
    f32 = jnp.float32

    low_rows = 2 * SPAN
    items = (
        (couple, cs, cr, half // 2, 2, 0, 0),
        (low, ls, lr, low_rows, width // low_rows, root, 0),
        (top, ts, tr, SPAN, top_pieces, 0, 0),
        (tile, gs, gr, SPAN, top_pieces, root, offset // SPAN),
    )

    def rel(item):
        return seen_from(row, items[item][5], rows_n)

    def place(item):
        return ring_pos(rel(item) // pair, chain)

    def far(item, way):
        at = place(item)
        return at if way == 0 else (chain - at) % chain

    def p_copy(item, kind, at, view, target):
        buffer, send, recv, count = items[item][:4]
        return pltpu.make_async_remote_copy(
            src_ref=view,
            dst_ref=buffer.at[pl.ds(at * count, count)],
            send_sem=send.at[kind, at],
            recv_sem=recv.at[at],
            device_id=(target, col),
            device_id_type=MESH,
        )

    def p_next(item, way):
        at = (place(item) + (1 if way == 0 else chain - 1)) % chain
        return placed_from(ring_at(at, chain) * pair, items[item][5], rows_n)

    def p_twin(item):
        return placed_from(rel(item) + pair - 1, items[item][5], rows_n)

    def p_held(item, at):
        buffer, count = items[item][0], items[item][3]
        return buffer.at[pl.ds(at * count, count)]

    def p_send(item, way, at, view):
        if chain > 1:
            @pl.when(far(item, way) != chain - 1)
            def _():
                p_copy(item, 0, at, view, p_next(item, way)).start()

        if pair > 1:
            p_copy(item, 1, at, view, p_twin(item)).start()

    def p_first(item, way, at):
        count = items[item][3]
        if item == COUPLE:
            p_send(item, way, at, l_ref.at[pl.ds(half + at * count, count), pl.ds(0, half)])
        elif item == LOWER:
            p_send(item, way, at, l_ref.at[pl.ds(offset + at * count, count)])
        elif item == TOP:
            @pl.when(panel)
            def _():
                p_send(item, way, at, a_ref.at[pl.ds(at * count, count)])

            @pl.when(jnp.logical_not(panel))
            def _():
                p_send(item, way, at, top.at[pl.ds(at * count, count)])
        else:
            p_send(item, way, at, zbuf.at[pl.ds(offset + at * count, count)])

    def wanted(item):
        return col != 0 if item in (LOWER, TILEROWS) else col >= 0

    def p_step(item, i):
        count, start = items[item][4], items[item][6]
        for way in range(2):
            stage = far(item, way) + rel(item) % pair
            at = i - start - stage * LAG

            @pl.when(
                jnp.logical_and(wanted(item), jnp.logical_and(jnp.logical_and(at >= 0, at < count), at % 2 == way))
            )
            def _():
                @pl.when(rel(item) == 0)
                def _():
                    p_first(item, way, at)

                @pl.when(rel(item) != 0)
                def _():
                    p_copy(item, 0, at, p_held(item, at), row).wait_recv()

                    @pl.when(rel(item) % pair == 0)
                    def _():
                        p_send(item, way, at, p_held(item, at))

    def p_finish(item):
        count = items[item][4]

        @pl.when(jnp.logical_and(wanted(item), rel(item) % pair == 0))
        def _():
            @pl.loop(0, count)
            def _(at):
                for way in range(2):
                    if chain > 1:
                        @pl.when(jnp.logical_and(at % 2 == way, far(item, way) != chain - 1))
                        def _():
                            p_copy(item, 0, at, p_held(item, at), row).wait_send()

                if pair > 1:
                    p_copy(item, 1, at, p_held(item, at), row).wait_send()

    def z_copy(i, source, target):
        return pltpu.make_async_remote_copy(
            src_ref=source.at[pl.ds(i * SPAN, SPAN)],
            dst_ref=target.at[pl.ds(i * SPAN, SPAN)],
            send_sem=zs.at[i],
            recv_sem=zr.at[i],
            device_id=(row, jnp.minimum(col + 1, cols_n - 1)),
            device_id_type=MESH,
        )

    def z_first(i):
        is_top = jnp.logical_and(row == 0, i < top_pieces)

        @pl.when(is_top)
        def _():
            z_copy(i, a_ref, top).start()

        @pl.when(jnp.logical_not(is_top))
        def _():
            z_copy(i, a_ref, zbuf).start()

    def z_step(i):
        is_top = jnp.logical_and(row == 0, i < top_pieces)

        @pl.when(panel)
        def _():
            z_copy(i, a_ref, zbuf).wait_send()

            @pl.when(i + AHEAD < pieces)
            def _():
                z_first(i + AHEAD)

        for mine, buffer in ((is_top, top), (jnp.logical_not(is_top), zbuf)):
            @pl.when(jnp.logical_and(col != 0, mine))
            def _():
                z_copy(i, buffer, buffer).wait_recv()

                @pl.when(relays)
                def _():
                    z_copy(i, buffer, buffer).start()

    def l_load(b):
        return pltpu.make_async_copy(
            l_ref.at[pl.ds(b * tile_n, tile_n)], out_ref.at[pl.ds(b * tile_n, tile_n)], here.at[b]
        )

    def base_load(b):
        return pltpu.make_async_copy(
            a_ref.at[pl.ds(b * tile_n, tile_n)], out_ref.at[pl.ds(b * tile_n, tile_n)], here.at[blocks + b]
        )

    def a_load(b):
        return pltpu.make_async_copy(
            a_ref.at[pl.ds(b * tile_n, tile_n)], zbuf.at[pl.ds(b * tile_n, tile_n)], here.at[2 * blocks + b]
        )

    extra = 3 * blocks
    inv_load = [
        pltpu.make_async_copy(
            i_ref.at[k], work.at[pl.ds(k * half, half), pl.ds(k * half, half)], here.at[extra + k]
        )
        for k in range(2)
    ]
    couple_load = pltpu.make_async_copy(l_ref.at[pl.ds(half, half), pl.ds(0, half)], couple, here.at[extra + 2])
    low_load = pltpu.make_async_copy(l_ref.at[pl.ds(offset, width)], low, here.at[extra + 3])
    top_load = pltpu.make_async_copy(a_ref.at[pl.ds(0, width)], top, here.at[extra + 4])
    is_root = jnp.logical_and(row == root, col != 0)
    first_top = jnp.logical_and(row == 0, panel)

    for copy in inv_load:
        copy.start()

    @pl.loop(0, blocks)
    def _(b):
        l_load(b).start()

    barrier = pltpu.get_barrier_semaphore()
    for step in range(1, rows_n):
        pl.semaphore_signal(barrier, inc=1, device_id=((row + step) % rows_n, col), device_id_type=MESH)

    @pl.when(col != cols_n - 1)
    def _():
        pl.semaphore_signal(
            barrier, inc=1, device_id=(row, jnp.minimum(col + 1, cols_n - 1)), device_id_type=MESH
        )

    @pl.when(col != 0)
    def _():
        pl.semaphore_signal(barrier, inc=1, device_id=(row, jnp.maximum(col - 1, 0)), device_id_type=MESH)

    ends = jnp.where(col == 0, 1, 0) + jnp.where(col == cols_n - 1, 1, 0)
    pl.semaphore_wait(barrier, rows_n + 1 - ends)

    if cols_n > 1:
        @pl.when(panel)
        def _():
            @pl.loop(0, min(AHEAD, pieces))
            def _(i):
                z_first(i)

    @pl.when(row == 0)
    def _():
        couple_load.start()

    @pl.when(is_root)
    def _():
        low_load.start()

    @pl.when(first_top)
    def _():
        top_load.start()

    @pl.when(panel)
    def _():
        @pl.loop(0, blocks)
        def _(b):
            a_load(b).start()

    def minus_eye(at, count):
        rows = lax.broadcasted_iota(jnp.int32, (count, width), 0) + at
        columns = lax.broadcasted_iota(jnp.int32, (count, width), 1)
        return jnp.where(rows == columns, -1.0, 0.0)

    strip = min(64, tile_n)
    strips = depth // strip

    def l_piece(i):
        per = tile_n // strip
        b = i // per
        rows = pl.ds(pl.multiple_of(i * strip, strip), strip)
        block = pl.ds(pl.multiple_of(b * tile_n, tile_n), tile_n)

        @pl.when(i % per == 0)
        def _():
            l_load(b).wait()

        is_top = jnp.logical_and(row == 0, i * strip < width)

        @pl.when(is_top)
        def _():
            lh[rows] = jnp.where(panel, minus_eye(i * strip, strip), 0.0).astype(jnp.bfloat16)
            ll[rows] = jnp.zeros((strip, width), jnp.bfloat16)

        @pl.when(jnp.logical_not(is_top))
        def _():
            lh[rows], ll[rows] = split(out_ref[rows])

        @pl.when(i % per == per - 1)
        def _():
            @pl.when(panel)
            def _():
                out_ref[block] = jnp.zeros((tile_n, width), f32)

            @pl.when(jnp.logical_not(panel))
            def _():
                base_load(b).start()

    def corner_piece(k):
        count = half // small

        @pl.when(k == 0)
        def _():
            for copy in inv_load:
                copy.wait()

            @pl.when(row == 0)
            def _():
                couple_load.wait()

            work[0:half, half:] = jnp.zeros((half, width - half), f32)

        rows = pl.ds(pl.multiple_of((k % count) * small, small), small)
        lower_rows = pl.ds(pl.multiple_of(half + (k % count) * small, small), small)

        @pl.when(k < count)
        def _():
            part[rows] = full_dot(couple[rows], work[0:half, 0:half])

        @pl.when(k >= count)
        def _():
            work[lower_rows, 0:half] = -full_dot(work[lower_rows, half:], part[...])

    def rows_of(b):
        return pl.ds(pl.multiple_of(b * tile_n, tile_n), tile_n)

    def inv_piece(b):
        ih[rows_of(b)], il[rows_of(b)] = split(work[rows_of(b)])

    def key_piece(b):
        @pl.when(b == 0)
        def _():
            @pl.when(is_root)
            def _():
                low_load.wait()

            @pl.loop(0, blocks)
            def _(k):
                @pl.when(jnp.logical_not(panel))
                def _():
                    base_load(k).wait()

                @pl.when(panel)
                def _():
                    a_load(k).wait()

        @pl.when(panel)
        def _():
            low[rows_of(b)] = minus_eye(b * tile_n, tile_n)

        for n in range(groups):
            at = n * tile_n
            columns = slice(at, at + tile_n)
            high, rest = split(low[rows_of(b), at:])
            kh[rows_of(b), columns], kl[rows_of(b), columns] = split(
                dot3(high, rest, ih[at:, columns], il[at:, columns], NN)
            )

    def row_piece(h):
        b, side = h // 2, h % 2

        @pl.when(jnp.logical_not(jnp.logical_and(row == 0, b * tile_n < width)))
        def _():
            columns = pl.ds(pl.multiple_of(side * (width // 2), width // 2), width // 2)
            high, rest = split(zbuf[rows_of(b)])
            out_ref[rows_of(b), columns] -= dot3(high, rest, kh[columns], kl[columns], NT)

    def top_piece(b):
        @pl.when(jnp.logical_and(first_top, b == 0))
        def _():
            top_load.wait()

        ch[rows_of(b)], cl[rows_of(b)] = split(top[rows_of(b)])

    def product_piece(h):
        b, side = h // 2, h % 2
        columns = pl.ds(pl.multiple_of(side * (width // 2), width // 2), width // 2)
        high, rest = kh[rows_of(b)], kl[rows_of(b)]
        work[rows_of(b), columns] = dot3(high, rest, ch[columns], cl[columns], NT)

        @pl.when(jnp.logical_not(panel))
        def _():
            work[rows_of(b), columns] = 0.5 * (
                work[rows_of(b), columns] + dot3(high, rest, ch[:, columns], cl[:, columns], NN)
            )

    def weight_piece(j):
        own = pl.ds(pl.multiple_of((offset + j * tile_n) % depth, tile_n), tile_n)
        mine = jnp.where(row == root, zbuf[own], tile[rows_of(j)])
        high, rest = split(jnp.where(panel, 0.0, mine) - work[rows_of(j)])
        for n in range(groups):
            at, end = n * tile_n, (n + 1) * tile_n
            vh[:, at:end], vl[:, at:end] = split(
                dot3(high[:, :end], rest[:, :end], ih[at:end, :end], il[at:end, :end], NT)
            )

    big = min(2 * tile_n, depth)

    def column_piece(j, k):
        rows = pl.ds(pl.multiple_of(k * big, big), big)
        columns = pl.ds(pl.multiple_of(j * tile_n, tile_n), tile_n)
        out_ref[rows, columns] -= dot3(lh[rows], ll[rows], vh[...], vl[...], NT)

    corner_at = 2 + most * LAG
    corner_n = 2 * (half // small)
    inv_at = corner_at + corner_n
    key_at = max(inv_at + groups, width // low_rows + most * LAG, strips)
    row_at = key_at + groups
    caught = 0
    while caught < blocks and per_block * (caught + 1) <= row_at + 2 * caught:
        caught += 1
    top_at = max(row_at + 2 * caught, top_pieces + most * LAG)
    product_at = top_at + groups
    weight_from = product_at + 2 * groups
    column_n = depth // big
    tile_from = offset // SPAN + most * LAG
    last_tile = (depth - width) // SPAN + most * LAG
    window = 1 + column_n
    weight_starts = [
        jnp.maximum(weight_from + window * j, tile_from + per_block * (j + 1)) for j in range(groups)
    ]
    steps = max(
        pieces + 2,
        max(weight_from + window * (groups - 1), last_tile + per_block * groups) + window,
        top_at + groups,
    )

    def between(i, start, count):
        return jnp.logical_and(i >= start, i < start + count)

    @pl.loop(0, steps)
    def _(i):
        if cols_n > 1:
            @pl.when(i < pieces)
            def _():
                z_step(i)

        if rows_n > 1:
            for item in range(4):
                p_step(item, i)

        for start, count, piece in (
            (0, strips, l_piece),
            (corner_at, corner_n, corner_piece),
            (inv_at, groups, inv_piece),
            (key_at, groups, key_piece),
            (top_at, groups, top_piece),
            (product_at, 2 * groups, product_piece),
        ):
            @pl.when(between(i, start, count))
            def _(start=start, piece=piece):
                piece(i - start)

        late = i // per_block - 1
        early = between(i, row_at, 2 * caught)
        in_time = jnp.logical_and(i % per_block < 2, jnp.logical_and(late >= caught, late < blocks))

        @pl.when(jnp.logical_or(early, in_time))
        def _():
            row_piece(jnp.where(early, i - row_at, 2 * late + i % per_block))

        group, at, busy = 0, 0, 0
        for j in range(groups):
            mine = between(i, weight_starts[j], window)
            group = group + jnp.where(mine, j, 0)
            at = at + jnp.where(mine, i - weight_starts[j], 0)
            busy = busy + jnp.where(mine, 1, 0)

        @pl.when(jnp.logical_and(busy > 0, at == 0))
        def _():
            weight_piece(group)

        @pl.when(jnp.logical_and(busy > 0, at > 0))
        def _():
            column_piece(group, at - 1)

    if cols_n > 1:
        @pl.when(relays)
        def _():
            @pl.loop(0, pieces)
            def _(i):
                z_copy(i, zbuf, zbuf).wait_send()

    if rows_n > 1:
        for item in range(4):
            p_finish(item)


def body(rows_n, cols_n, a_window, l_panel, l_inverse):
    depth, width = a_window.shape
    half = l_inverse.shape[1]
    f32, bf16 = jnp.float32, jnp.bfloat16
    tile_n = min(TILE, width)
    dma = pltpu.SemaphoreType.DMA
    pieces, top_pieces, low_pieces = depth // SPAN, width // SPAN, width // (2 * SPAN)
    square = pltpu.VMEM((width, width), f32)
    narrow = pltpu.VMEM((width, width), bf16)
    return pl.pallas_call(
        functools.partial(step_kernel, rows_n, cols_n),
        out_shape=pltpu.VMEM((depth, width), f32),
        in_specs=[pl.BlockSpec(memory_space=pl.ANY)] * 3,
        out_specs=pl.BlockSpec(memory_space=pltpu.VMEM),
        scratch_shapes=[
            pltpu.VMEM((depth, width), f32),
            square,
            square,
            square,
            pltpu.VMEM((half, half), f32),
            pltpu.VMEM((half, half), f32),
            square,
            pltpu.VMEM((depth, width), bf16),
            pltpu.VMEM((depth, width), bf16),
            narrow,
            narrow,
            narrow,
            narrow,
            narrow,
            narrow,
            pltpu.VMEM((tile_n, width), bf16),
            pltpu.VMEM((tile_n, width), bf16),
            dma((pieces,)),
            dma((pieces,)),
            dma((2, 2)),
            dma((2,)),
            dma((2, low_pieces)),
            dma((low_pieces,)),
            dma((2, top_pieces)),
            dma((top_pieces,)),
            dma((2, top_pieces)),
            dma((top_pieces,)),
            dma((3 * (depth // tile_n) + 5,)),
        ],
        compiler_params=pltpu.CompilerParams(
            collective_id=0, has_side_effects=True, vmem_limit_bytes=50 * 1024 * 1024
        ),
    )(a_window, l_panel, l_inverse)


def solution(mesh):
    placed = (P("row", "col"), P("row", None), P())
    return jax.shard_map(
        functools.partial(body, mesh.shape["row"], mesh.shape["col"]),
        mesh=mesh,
        in_specs=placed,
        out_specs=P("row", "col"),
        check_vma=False,
    )
```

```python
import functools

import jax
import jax.numpy as jnp
from jax import lax
from jax.experimental import pallas as pl
from jax.experimental.pallas import tpu as pltpu
from jax.sharding import PartitionSpec as P

MESH = pl.DeviceIdType.MESH
SPAN = 16
PACE = 2
TILE = 256
AHEAD = (2, 16)
LAGS = (4, 4, 4, 3)
LATER = (0, 4, 0, 36)
WAITS = (6, 6, 6, -8, -6)
NN, NT = ((1,), (0,)), ((1,), (1,))
COUPLE, LOWER, TOP, TILEROWS = range(4)


def bits_of(count):
    return max(count.bit_length() - 1, 0)


def ring_pos(index, count):
    if count & (count - 1):
        return index
    parity, place = 0, 0
    for bit in reversed(range(bits_of(count))):
        parity = (parity + (index // 2**bit) % 2) % 2
        place = place + parity * 2**bit
    return place


def ring_at(place, count):
    if count & (count - 1):
        return place
    index = 0
    for bit in range(bits_of(count)):
        index = index + (((place // 2**bit) % 2 + (place // 2 ** (bit + 1)) % 2) % 2) * 2**bit
    return index


def seen_from(index, root, count):
    if count & (count - 1):
        return (index - root + count) % count
    return sum((((index // 2**bit) % 2 + (root // 2**bit) % 2) % 2) * 2**bit for bit in range(bits_of(count)))


def placed_from(offset, root, count):
    if count & (count - 1):
        return (offset + root) % count
    return seen_from(offset, root, count)


def couple_parts(half):
    return max(half // (2 * PACE * SPAN), 2)


def split(value):
    high = value.astype(jnp.bfloat16)
    return high, (value - high.astype(jnp.float32)).astype(jnp.bfloat16)


def dot3(left_high, left_low, high, low, dims):
    total = lax.dot_general(left_high, high, (dims, ((), ())), preferred_element_type=jnp.float32)
    total += lax.dot_general(left_high, low, (dims, ((), ())), preferred_element_type=jnp.float32)
    return total + lax.dot_general(left_low, high, (dims, ((), ())), preferred_element_type=jnp.float32)


def full_dot(left, right):
    return lax.dot_general(
        left, right, (NN, ((), ())), precision=lax.Precision.HIGHEST, preferred_element_type=jnp.float32
    )


def step_kernel(
    rows_n, cols_n, a_ref, l_ref, i_ref, out_ref,
    zbuf, top, tile, low, couple, part, work, lh, ll, ih, il, kh, kl, ch, cl, vh, vl,
    zs, zr, cs, cr, ls, lr, ts, tr, gs, gr, here,
):
    row, col = lax.axis_index("row"), lax.axis_index("col")
    depth, width = a_ref.shape
    half = i_ref.shape[1]
    pieces = depth // SPAN
    top_pieces = width // SPAN
    tile_n = min(TILE, width)
    blocks, groups = depth // tile_n, width // tile_n
    per_block = tile_n // SPAN
    small = min(128, half)
    panel = col == 0
    relays = jnp.logical_and(col != 0, col != cols_n - 1)
    root = (col * width) // depth
    offset = (col * width) % depth
    pair = 2 if rows_n % 2 == 0 else 1
    chain = rows_n // pair
    f32 = jnp.float32

    low_rows, own_rows = 2 * PACE * SPAN, PACE * SPAN
    parts = couple_parts(half)
    natural = row == 0
    turned = depth // width - 1 - offset // width
    tile_at = jnp.where(root == 0, offset // width, turned) * top_pieces
    tile_start = jnp.where(tile_at > 0, tile_at, LATER[TILEROWS])

    def sent_at(index, per):
        return jnp.where(natural, index, (depth // width - 1 - index // per) * per + index % per)

    items = (
        (couple, cs, cr, half // parts, parts, 0, 0),
        (low, ls, lr, low_rows, width // low_rows, root, LATER[LOWER]),
        (top, ts, tr, own_rows, width // own_rows, 0, PACE - 1),
        (tile, gs, gr, own_rows, width // own_rows, root, tile_start + PACE - 1),
    )

    rel, far, is_last, level, p_next, p_twin = [], [], [], [], [], []
    for item in range(4):
        origin = items[item][5]
        seen = seen_from(row, origin, rows_n)
        at = ring_pos(seen // pair, chain)
        odd = seen % pair
        ways = (at, (chain - at) % chain)
        short = item == TILEROWS and chain > 2
        rel.append(seen)
        far.append(ways)
        is_last.append(tuple(way >= chain - (2 if short else 1) for way in ways))
        if item == TILEROWS:
            ways = tuple(jnp.where(way == chain - 1, jnp.minimum(way, 1), way) for way in ways)
        level.append(tuple(way + odd for way in ways))
        p_next.append(
            tuple(
                placed_from(ring_at((at + (1 if way == 0 else chain - 1)) % chain, chain) * pair, origin, rows_n)
                for way in range(2)
            )
        )
        p_twin.append(placed_from(seen + (pair - 1) * (1 - odd), origin, rows_n))

    def wait(item):
        if item != TILEROWS:
            return WAITS[item]
        return jnp.where(tile_at > 0, jnp.where(root == 0, WAITS[item], WAITS[item + 1]), 0)

    begins = [
        tuple(items[item][6] + jnp.where(of_way > 0, of_way * LAGS[item] + wait(item), 0) for of_way in level[item])
        for item in range(4)
    ]
    sends_on = [rel[item] % pair == 0 for item in range(4)]
    is_first = [rel[item] == 0 for item in range(4)]

    def most(item):
        chips = max(chain - 2, 1) if item == TILEROWS and chain > 1 else chain - 1
        return chips + pair - 1

    def p_copy(item, kind, at, source, first, columns, target):
        buffer, send, recv, count = items[item][:4]
        return pltpu.make_async_remote_copy(
            src_ref=source.at[pl.ds(first + at * count, count), columns],
            dst_ref=buffer.at[pl.ds(at * count, count), columns],
            send_sem=send.at[kind, at],
            recv_sem=recv.at[at],
            device_id=(target, col),
            device_id_type=MESH,
        )

    def upper(k):
        return pl.ds(k * tile_n, width - k * tile_n)

    def each(item, at, act):
        if item != TOP:
            act(pl.ds(0, items[item][0].shape[1]))
            return

        @pl.when(panel)
        def _():
            act(pl.ds(0, width))

        for k in range(groups):
            @pl.when(jnp.logical_and(jnp.logical_not(panel), at // (tile_n // own_rows) == k))
            def _(k=k):
                act(upper(k))

    def p_send(item, way, at, source, first, columns):
        if chain > 1:
            @pl.when(jnp.logical_not(is_last[item][way]))
            def _():
                p_copy(item, 0, at, source, first, columns, p_next[item][way]).start()

        if chain > 2 and item == TILEROWS:
            @pl.when(is_first[item])
            def _():
                p_copy(item, 2, at, source, first, columns, p_next[item][1 - way]).start()

        if pair > 1:
            p_copy(item, 1, at, source, first, columns, p_twin[item]).start()

    def p_first(item, way, at, columns):
        if item == COUPLE:
            p_send(item, way, at, l_ref, half, columns)
        elif item == LOWER:
            p_send(item, way, at, l_ref, offset, columns)
        elif item == TOP:
            @pl.when(panel)
            def _():
                p_send(item, way, at, a_ref, 0, columns)

            @pl.when(jnp.logical_not(panel))
            def _():
                p_send(item, way, at, top, 0, columns)
        else:
            p_send(item, way, at, zbuf, offset, columns)

    wanted = [col != 0 if item in (LOWER, TILEROWS) else col >= 0 for item in range(4)]

    def p_step(item, i):
        count = items[item][4]
        for way in range(2):
            since = i - begins[item][way]
            at = since // PACE

            @pl.when(
                jnp.logical_and(wanted[item], jnp.logical_and(jnp.logical_and(since >= 0, at < count), since % (2 * PACE) == way * PACE))
            )
            def _():
                def act(columns):
                    @pl.when(is_first[item])
                    def _():
                        p_first(item, way, at, columns)

                    @pl.when(jnp.logical_not(is_first[item]))
                    def _():
                        buffer = items[item][0]
                        p_copy(item, 0, at, buffer, 0, columns, row).wait_recv()

                        @pl.when(sends_on[item])
                        def _():
                            p_send(item, way, at, buffer, 0, columns)

                each(item, at, act)

    def p_finish(item):
        buffer, count = items[item][0], items[item][4]

        @pl.when(jnp.logical_and(wanted[item], sends_on[item]))
        def _():
            @pl.loop(0, count)
            def _(at):
                def act(columns):
                    for way in range(2):
                        if chain > 1:
                            @pl.when(jnp.logical_and(at % 2 == way, jnp.logical_not(is_last[item][way])))
                            def _():
                                p_copy(item, 0, at, buffer, 0, columns, row).wait_send()

                    if chain > 2 and item == TILEROWS:
                        @pl.when(is_first[item])
                        def _():
                            p_copy(item, 2, at, buffer, 0, columns, row).wait_send()

                    if pair > 1:
                        p_copy(item, 1, at, buffer, 0, columns, row).wait_send()

                each(item, at, act)

    def z_copy(i, source, target, columns):
        rows = pl.ds(pl.multiple_of(sent_at(i, top_pieces) * SPAN, SPAN), SPAN)
        return pltpu.make_async_remote_copy(
            src_ref=source.at[rows, columns],
            dst_ref=target.at[rows, columns],
            send_sem=zs.at[i],
            recv_sem=zr.at[i],
            device_id=(row, jnp.minimum(col + 1, cols_n - 1)),
            device_id_type=MESH,
        )

    def z_each(i, act):
        is_top = jnp.logical_and(row == 0, i < top_pieces)
        for k in range(groups):
            @pl.when(jnp.logical_and(is_top, i // per_block == k))
            def _(k=k):
                act(tile, top, upper(k))

        @pl.when(jnp.logical_not(is_top))
        def _():
            act(a_ref, zbuf, pl.ds(0, width))

    ahead = jnp.where(row == 0, AHEAD[0], AHEAD[1])

    def z_first(i):
        z_each(i, lambda source, target, columns: z_copy(i, source, target, columns).start())

    def z_step(i):
        @pl.when(panel)
        def _():
            z_each(i, lambda source, target, columns: z_copy(i, source, target, columns).wait_send())

            @pl.when(i + ahead < pieces)
            def _():
                z_first(i + ahead)

        @pl.when(col != 0)
        def _():
            def act(source, target, columns):
                z_copy(i, target, target, columns).wait_recv()

                @pl.when(relays)
                def _():
                    z_copy(i, target, target, columns).start()

            z_each(i, act)

    def l_load(b):
        return pltpu.make_async_copy(
            l_ref.at[pl.ds(b * tile_n, tile_n)], out_ref.at[pl.ds(b * tile_n, tile_n)], here.at[b]
        )

    def base_load(b):
        return pltpu.make_async_copy(
            a_ref.at[pl.ds(b * tile_n, tile_n)], out_ref.at[pl.ds(b * tile_n, tile_n)], here.at[blocks + b]
        )

    def a_load(b):
        return pltpu.make_async_copy(
            a_ref.at[pl.ds(b * tile_n, tile_n)], zbuf.at[pl.ds(b * tile_n, tile_n)], here.at[2 * blocks + b]
        )

    extra = 3 * blocks
    inv_load = [
        pltpu.make_async_copy(
            i_ref.at[k], work.at[pl.ds(k * half, half), pl.ds(k * half, half)], here.at[extra + k]
        )
        for k in range(2)
    ]
    couple_load = pltpu.make_async_copy(l_ref.at[pl.ds(half, half), pl.ds(0, half)], couple, here.at[extra + 2])
    low_load = pltpu.make_async_copy(l_ref.at[pl.ds(offset, width)], low, here.at[extra + 3])
    top_load = pltpu.make_async_copy(a_ref.at[pl.ds(0, width)], top, here.at[extra + 4])
    is_root = jnp.logical_and(row == root, col != 0)
    first_top = jnp.logical_and(row == 0, panel)

    @pl.when(first_top)
    def _():
        top_load.start()

    for copy in inv_load:
        copy.start()

    @pl.loop(0, blocks)
    def _(b):
        l_load(b).start()

    barrier = pltpu.get_barrier_semaphore()
    for step in range(1, rows_n):
        pl.semaphore_signal(barrier, inc=1, device_id=((row + step) % rows_n, col), device_id_type=MESH)

    @pl.when(col != cols_n - 1)
    def _():
        pl.semaphore_signal(
            barrier, inc=1, device_id=(row, jnp.minimum(col + 1, cols_n - 1)), device_id_type=MESH
        )

    @pl.when(col != 0)
    def _():
        pl.semaphore_signal(barrier, inc=1, device_id=(row, jnp.maximum(col - 1, 0)), device_id_type=MESH)

    ends = jnp.where(col == 0, 1, 0) + jnp.where(col == cols_n - 1, 1, 0)
    pl.semaphore_wait(barrier, rows_n + 1 - ends)

    @pl.when(first_top)
    def _():
        top_load.wait()
        for k in range(groups):
            rows = slice(k * tile_n, (k + 1) * tile_n)
            for n in range(k, groups):
                columns = slice(n * tile_n, (n + 1) * tile_n)
                tile[rows, columns] = top[rows, columns] + top[columns, rows].T

    if cols_n > 1:
        @pl.when(panel)
        def _():
            @pl.loop(0, jnp.minimum(ahead, pieces))
            def _(i):
                z_first(i)

    @pl.when(row == 0)
    def _():
        couple_load.start()

    @pl.when(is_root)
    def _():
        low_load.start()

    @pl.when(panel)
    def _():
        @pl.loop(0, blocks)
        def _(b):
            a_load(b).start()

    def minus_eye(at, count):
        rows = lax.broadcasted_iota(jnp.int32, (count, width), 0) + at
        columns = lax.broadcasted_iota(jnp.int32, (count, width), 1)
        return jnp.where(rows == columns, -1.0, 0.0)

    strip = min(64, tile_n)
    strips = depth // strip

    def l_piece(i):
        per = tile_n // strip
        b = i // per
        rows = pl.ds(pl.multiple_of(i * strip, strip), strip)
        block = pl.ds(pl.multiple_of(b * tile_n, tile_n), tile_n)

        @pl.when(i % per == 0)
        def _():
            l_load(b).wait()

        is_top = jnp.logical_and(row == 0, i * strip < width)

        @pl.when(is_top)
        def _():
            lh[rows] = jnp.where(panel, minus_eye(i * strip, strip), 0.0).astype(jnp.bfloat16)
            ll[rows] = jnp.zeros((strip, width), jnp.bfloat16)

        @pl.when(jnp.logical_not(is_top))
        def _():
            lh[rows], ll[rows] = split(out_ref[rows])

        @pl.when(i % per == per - 1)
        def _():
            @pl.when(panel)
            def _():
                out_ref[block] = jnp.zeros((tile_n, width), f32)

            @pl.when(jnp.logical_not(panel))
            def _():
                base_load(b).start()

    def corner_piece(k):
        count = half // small

        @pl.when(k == 0)
        def _():
            for copy in inv_load:
                copy.wait()

            @pl.when(row == 0)
            def _():
                couple_load.wait()

            work[0:half, half:] = jnp.zeros((half, width - half), f32)

        rows = pl.ds(pl.multiple_of((k % count) * small, small), small)
        lower_rows = pl.ds(pl.multiple_of(half + (k % count) * small, small), small)

        @pl.when(k < count)
        def _():
            part[rows] = full_dot(couple[rows], work[0:half, 0:half])

        @pl.when(k >= count)
        def _():
            work[lower_rows, 0:half] = -full_dot(work[lower_rows, half:], part[...])

    def rows_of(b):
        return pl.ds(pl.multiple_of(b * tile_n, tile_n), tile_n)

    def inv_piece(b):
        ih[rows_of(b)], il[rows_of(b)] = split(work[rows_of(b)])

    def key_piece(b):
        @pl.when(b == 0)
        def _():
            @pl.when(is_root)
            def _():
                low_load.wait()

            @pl.loop(0, blocks)
            def _(k):
                @pl.when(jnp.logical_not(panel))
                def _():
                    base_load(k).wait()

                @pl.when(panel)
                def _():
                    a_load(k).wait()

        @pl.when(panel)
        def _():
            low[rows_of(b)] = minus_eye(b * tile_n, tile_n)

        for n in range(groups):
            at = n * tile_n
            columns = slice(at, at + tile_n)
            high, rest = split(low[rows_of(b), at:])
            kh[rows_of(b), columns], kl[rows_of(b), columns] = split(
                dot3(high, rest, ih[at:, columns], il[at:, columns], NN)
            )

    def row_piece(h):
        b, side = sent_at(h // 2, groups), h % 2

        @pl.when(jnp.logical_not(jnp.logical_and(row == 0, b * tile_n < width)))
        def _():
            columns = pl.ds(pl.multiple_of(side * (width // 2), width // 2), width // 2)
            high, rest = split(zbuf[rows_of(b)])
            out_ref[rows_of(b), columns] -= dot3(high, rest, kh[columns], kl[columns], NT)

    def top_piece(b):
        ch[rows_of(b)], cl[rows_of(b)] = split(top[rows_of(b)])

    def product_piece(h):
        b, group = h // groups, h % groups
        high, rest = kh.at[rows_of(b)], kl.at[rows_of(b)]
        for n in range(groups):
            own, at = slice(n * tile_n, (n + 1) * tile_n), (n + 1) * tile_n

            @pl.when(jnp.logical_and(group == n, panel))
            def _():
                work[rows_of(b), own] = dot3(high[...], rest[...], ch[own], cl[own], NT)

            @pl.when(jnp.logical_and(group == n, jnp.logical_not(panel)))
            def _():
                total = dot3(high[:, :at], rest[:, :at], ch[:at, own], cl[:at, own], NN)
                if n + 1 < groups:
                    total += dot3(high[:, at:], rest[:, at:], ch[own, at:], cl[own, at:], NT)
                work[rows_of(b), own] = 0.5 * total

    def weight_piece(j):
        own = pl.ds(pl.multiple_of((offset + j * tile_n) % depth, tile_n), tile_n)
        for mine, source, rows in ((row == root, zbuf, own), (row != root, tile, rows_of(j))):
            @pl.when(mine)
            def _(source=source, rows=rows):
                vh[...], vl[...] = split(jnp.where(panel, 0.0, source[rows]) - work[rows_of(j)])

        for n in reversed(range(groups)):
            at, end = n * tile_n, (n + 1) * tile_n
            vh[:, at:end], vl[:, at:end] = split(
                dot3(vh[:, :end], vl[:, :end], ih[at:end, :end], il[at:end, :end], NT)
            )

    big = min(2 * tile_n, depth)

    def column_piece(j, k):
        rows = pl.ds(pl.multiple_of(k * big, big), big)
        columns = pl.ds(pl.multiple_of(j * tile_n, tile_n), tile_n)
        out_ref[rows, columns] -= dot3(lh[rows], ll[rows], vh[...], vl[...], NT)

    corner_at = PACE * parts + most(COUPLE) * LAGS[COUPLE] + WAITS[COUPLE]
    corner_n = 2 * (half // small)
    inv_at = corner_at + corner_n
    key_at = max(inv_at + groups, LATER[LOWER] + PACE * (width // low_rows) + most(LOWER) * LAGS[LOWER] + WAITS[LOWER], strips)
    row_at = key_at + groups
    caught = 0
    while caught < blocks and per_block * (caught + 1) <= row_at + 2 * caught:
        caught += 1
    top_at = max(row_at + 2 * caught, PACE - 1 + top_pieces + most(TOP) * LAGS[TOP] + WAITS[TOP])
    product_at = top_at + groups
    weight_from = product_at + groups * groups
    column_n = depth // big
    tile_from = tile_start + PACE - 1 + jnp.maximum(0, most(TILEROWS) * LAGS[TILEROWS] + wait(TILEROWS))
    last_tile = PACE - 1 + max((depth - width) // SPAN, LATER[TILEROWS]) + most(TILEROWS) * LAGS[TILEROWS] + max(WAITS[TILEROWS], 0)
    window = 1 + column_n
    weight_starts = [
        jnp.maximum(weight_from + window * j, tile_from + per_block * (j + 1)) for j in range(groups)
    ]
    steps = max(
        pieces + 2,
        max(weight_from + window * (groups - 1), last_tile + per_block * groups) + window,
        top_at + groups,
    )

    def between(i, start, count):
        return jnp.logical_and(i >= start, i < start + count)

    @pl.loop(0, steps)
    def _(i):
        if cols_n > 1:
            @pl.when(i < pieces)
            def _():
                z_step(i)

        if rows_n > 1:
            for item in range(4):
                p_step(item, i)

        for start, count, piece in (
            (0, strips, l_piece),
            (corner_at, corner_n, corner_piece),
            (inv_at, groups, inv_piece),
            (key_at, groups, key_piece),
            (top_at, groups, top_piece),
            (product_at, groups * groups, product_piece),
        ):
            @pl.when(between(i, start, count))
            def _(start=start, piece=piece):
                piece(i - start)

        late = i // per_block - 1
        early = between(i, row_at, 2 * caught)
        in_time = jnp.logical_and(i % per_block < 2, jnp.logical_and(late >= caught, late < blocks))

        @pl.when(jnp.logical_or(early, in_time))
        def _():
            row_piece(jnp.where(early, i - row_at, 2 * late + i % per_block))

        group, at, busy = 0, 0, 0
        for j in range(groups):
            mine = between(i, weight_starts[j], window)
            group = group + jnp.where(mine, j, 0)
            at = at + jnp.where(mine, i - weight_starts[j], 0)
            busy = busy + jnp.where(mine, 1, 0)

        @pl.when(jnp.logical_and(busy > 0, at == 0))
        def _():
            weight_piece(group)

        @pl.when(jnp.logical_and(busy > 0, at > 0))
        def _():
            column_piece(group, at - 1)

    if cols_n > 1:
        @pl.when(relays)
        def _():
            @pl.loop(0, pieces)
            def _(i):
                z_each(i, lambda source, target, columns: z_copy(i, target, target, columns).wait_send())

    if rows_n > 1:
        for item in range(4):
            p_finish(item)


def body(rows_n, cols_n, a_window, l_panel, l_inverse):
    depth, width = a_window.shape
    half = l_inverse.shape[1]
    f32, bf16 = jnp.float32, jnp.bfloat16
    tile_n = min(TILE, width)
    dma = pltpu.SemaphoreType.DMA
    pieces, top_pieces, low_pieces = depth // SPAN, width // (PACE * SPAN), width // (2 * PACE * SPAN)
    square = pltpu.VMEM((width, width), f32)
    narrow = pltpu.VMEM((width, width), bf16)
    return pl.pallas_call(
        functools.partial(step_kernel, rows_n, cols_n),
        out_shape=pltpu.VMEM((depth, width), f32),
        in_specs=[pl.BlockSpec(memory_space=pl.ANY)] * 3,
        out_specs=pl.BlockSpec(memory_space=pltpu.VMEM),
        scratch_shapes=[
            pltpu.VMEM((depth, width), f32),
            square,
            square,
            square,
            pltpu.VMEM((half, half), f32),
            pltpu.VMEM((half, half), f32),
            square,
            pltpu.VMEM((depth, width), bf16),
            pltpu.VMEM((depth, width), bf16),
            narrow,
            narrow,
            narrow,
            narrow,
            narrow,
            narrow,
            pltpu.VMEM((tile_n, width), bf16),
            pltpu.VMEM((tile_n, width), bf16),
            dma((pieces,)),
            dma((pieces,)),
            dma((2, couple_parts(half))),
            dma((couple_parts(half),)),
            dma((2, low_pieces)),
            dma((low_pieces,)),
            dma((2, top_pieces)),
            dma((top_pieces,)),
            dma((3, top_pieces)),
            dma((top_pieces,)),
            dma((3 * (depth // tile_n) + 5,)),
        ],
        compiler_params=pltpu.CompilerParams(
            collective_id=0, has_side_effects=True, vmem_limit_bytes=50 * 1024 * 1024
        ),
    )(a_window, l_panel, l_inverse)


def solution(mesh):
    placed = (P("row", "col"), P("row", None), P())
    return jax.shard_map(
        functools.partial(body, mesh.shape["row"], mesh.shape["col"]),
        mesh=mesh,
        in_specs=placed,
        out_specs=P("row", "col"),
        check_vma=False,
    )
```

```python
import functools

import jax
import jax.numpy as jnp
from jax import lax
from jax.experimental import pallas as pl
from jax.experimental.pallas import tpu as pltpu
from jax.sharding import PartitionSpec as P

MESH = pl.DeviceIdType.MESH
SPAN = 16
PACE = 2
TILE = 256
RECENT = 8
BEHIND = 12
AHEAD = (3, 24)
LAGS = (4, 4, 4, 3)
LATER = (0, 4, 0, 36)
WAITS = (6, 6, 6, -10, -4)
NN, NT = ((1,), (0,)), ((1,), (1,))
COUPLE, LOWER, TOP, TILEROWS = range(4)


def bits_of(count):
    return max(count.bit_length() - 1, 0)


def ring_pos(index, count):
    if count & (count - 1):
        return index
    parity, place = 0, 0
    for bit in reversed(range(bits_of(count))):
        parity = (parity + (index // 2**bit) % 2) % 2
        place = place + parity * 2**bit
    return place


def ring_at(place, count):
    if count & (count - 1):
        return place
    index = 0
    for bit in range(bits_of(count)):
        index = index + (((place // 2**bit) % 2 + (place // 2 ** (bit + 1)) % 2) % 2) * 2**bit
    return index


def seen_from(index, root, count):
    if count & (count - 1):
        return (index - root + count) % count
    return sum((((index // 2**bit) % 2 + (root // 2**bit) % 2) % 2) * 2**bit for bit in range(bits_of(count)))


def placed_from(offset, root, count):
    if count & (count - 1):
        return (offset + root) % count
    return seen_from(offset, root, count)


def couple_parts(half):
    return max(half // (2 * PACE * SPAN), 2)


def split(value):
    high = value.astype(jnp.bfloat16)
    return high, (value - high.astype(jnp.float32)).astype(jnp.bfloat16)


def dot3(left_high, left_low, high, low, dims):
    total = lax.dot_general(left_high, high, (dims, ((), ())), preferred_element_type=jnp.float32)
    total += lax.dot_general(left_high, low, (dims, ((), ())), preferred_element_type=jnp.float32)
    return total + lax.dot_general(left_low, high, (dims, ((), ())), preferred_element_type=jnp.float32)


def full_dot(left, right):
    return lax.dot_general(
        left, right, (NN, ((), ())), precision=lax.Precision.HIGHEST, preferred_element_type=jnp.float32
    )


def step_kernel(
    rows_n, cols_n, a_ref, l_ref, i_ref, out_ref,
    zbuf, top, tile, low, couple, part, work, lh, ll, ih, il, kh, kl, ch, cl, vh, vl,
    zs, zr, cs, cr, ls, lr, ts, tr, gs, gr, here,
):
    row, col = lax.axis_index("row"), lax.axis_index("col")
    depth, width = a_ref.shape
    half = i_ref.shape[1]
    pieces = depth // SPAN
    top_pieces = width // SPAN
    tile_n = min(TILE, width)
    blocks, groups = depth // tile_n, width // tile_n
    per_block = tile_n // SPAN
    small = min(128, half)
    panel = col == 0
    relays = jnp.logical_and(col != 0, col != cols_n - 1)
    root = (col * width) // depth
    offset = (col * width) % depth
    pair = 2 if rows_n % 2 == 0 else 1
    chain = rows_n // pair
    f32 = jnp.float32

    low_rows, own_rows = 2 * PACE * SPAN, PACE * SPAN
    parts = couple_parts(half)
    natural = row == 0
    turned = depth // width - 1 - offset // width
    tile_at = jnp.where(root == 0, offset // width, turned) * top_pieces
    tile_start = jnp.where(tile_at > 0, tile_at, LATER[TILEROWS])

    def sent_at(index, per):
        return jnp.where(natural, index, (depth // width - 1 - index // per) * per + index % per)

    items = (
        (couple, cs, cr, half // parts, parts, 0, 0),
        (low, ls, lr, low_rows, width // low_rows, root, LATER[LOWER]),
        (top, ts, tr, own_rows, width // own_rows, 0, PACE - 1),
        (tile, gs, gr, own_rows, width // own_rows, root, tile_start + PACE - 1),
    )

    rel, far, is_last, level, p_next, p_twin = [], [], [], [], [], []
    for item in range(4):
        origin = items[item][5]
        seen = seen_from(row, origin, rows_n)
        at = ring_pos(seen // pair, chain)
        odd = seen % pair
        ways = (at, (chain - at) % chain)
        short = item == TILEROWS and chain > 2
        rel.append(seen)
        far.append(ways)
        is_last.append(tuple(way >= chain - (2 if short else 1) for way in ways))
        if item == TILEROWS:
            ways = tuple(jnp.where(way == chain - 1, jnp.minimum(way, 1), way) for way in ways)
        level.append(tuple(way + odd for way in ways))
        p_next.append(
            tuple(
                placed_from(ring_at((at + (1 if way == 0 else chain - 1)) % chain, chain) * pair, origin, rows_n)
                for way in range(2)
            )
        )
        p_twin.append(placed_from(seen + (pair - 1) * (1 - odd), origin, rows_n))

    def wait(item):
        if item != TILEROWS:
            return WAITS[item]
        return jnp.where(tile_at > 0, jnp.where(root == 0, WAITS[item], WAITS[item + 1]), 0)

    begins = [
        tuple(items[item][6] + jnp.where(of_way > 0, of_way * LAGS[item] + wait(item), 0) for of_way in level[item])
        for item in range(4)
    ]
    sends_on = [rel[item] % pair == 0 for item in range(4)]
    is_first = [rel[item] == 0 for item in range(4)]

    def most(item):
        chips = max(chain - 2, 1) if item == TILEROWS and chain > 1 else chain - 1
        return chips + pair - 1

    def p_copy(item, kind, at, source, first, columns, target):
        buffer, send, recv, count = items[item][:4]
        return pltpu.make_async_remote_copy(
            src_ref=source.at[pl.ds(first + at * count, count), columns],
            dst_ref=buffer.at[pl.ds(at * count, count), columns],
            send_sem=send.at[kind, at],
            recv_sem=recv.at[at],
            device_id=(target, col),
            device_id_type=MESH,
        )

    def upper(k):
        return pl.ds(k * tile_n, width - k * tile_n)

    def each(item, at, act):
        if item != TOP:
            act(pl.ds(0, items[item][0].shape[1]))
            return

        @pl.when(panel)
        def _():
            act(pl.ds(0, width))

        for k in range(groups):
            @pl.when(jnp.logical_and(jnp.logical_not(panel), at // (tile_n // own_rows) == k))
            def _(k=k):
                act(upper(k))

    def p_send(item, way, at, source, first, columns):
        if chain > 1:
            @pl.when(jnp.logical_not(is_last[item][way]))
            def _():
                p_copy(item, 0, at, source, first, columns, p_next[item][way]).start()

        if chain > 2 and item == TILEROWS:
            @pl.when(is_first[item])
            def _():
                p_copy(item, 2, at, source, first, columns, p_next[item][1 - way]).start()

        if pair > 1:
            p_copy(item, 1, at, source, first, columns, p_twin[item]).start()

    def p_first(item, way, at, columns):
        if item == COUPLE:
            p_send(item, way, at, l_ref, half, columns)
        elif item == LOWER:
            p_send(item, way, at, l_ref, offset, columns)
        elif item == TOP:
            @pl.when(panel)
            def _():
                p_send(item, way, at, a_ref, 0, columns)

            @pl.when(jnp.logical_not(panel))
            def _():
                p_send(item, way, at, top, 0, columns)
        else:
            p_send(item, way, at, zbuf, offset, columns)

    wanted = [col != 0 if item in (LOWER, TILEROWS) else col >= 0 for item in range(4)]

    def p_step(item, i):
        count = items[item][4]
        for way in range(2):
            since = i - begins[item][way]
            at = since // PACE

            @pl.when(
                jnp.logical_and(wanted[item], jnp.logical_and(jnp.logical_and(since >= 0, at < count), since % (2 * PACE) == way * PACE))
            )
            def _():
                def act(columns):
                    @pl.when(is_first[item])
                    def _():
                        p_first(item, way, at, columns)

                    @pl.when(jnp.logical_not(is_first[item]))
                    def _():
                        buffer = items[item][0]
                        p_copy(item, 0, at, buffer, 0, columns, row).wait_recv()

                        @pl.when(sends_on[item])
                        def _():
                            p_send(item, way, at, buffer, 0, columns)

                each(item, at, act)

                if item == TILEROWS:
                    @pl.when(jnp.logical_and(sends_on[item], at >= RECENT))
                    def _():
                        p_sent(item, at - RECENT)

    def p_sent(item, at):
        buffer = items[item][0]

        def act(columns):
            for way in range(2):
                if chain > 1:
                    @pl.when(jnp.logical_and(at % 2 == way, jnp.logical_not(is_last[item][way])))
                    def _():
                        p_copy(item, 0, at, buffer, 0, columns, row).wait_send()

            if chain > 2 and item == TILEROWS:
                @pl.when(is_first[item])
                def _():
                    p_copy(item, 2, at, buffer, 0, columns, row).wait_send()

            if pair > 1:
                p_copy(item, 1, at, buffer, 0, columns, row).wait_send()

        each(item, at, act)

    def p_finish(item):
        held = RECENT if item == TILEROWS else items[item][4]

        @pl.when(jnp.logical_and(wanted[item], sends_on[item]))
        def _():
            @pl.loop(max(0, items[item][4] - held), items[item][4])
            def _(at):
                p_sent(item, at)

    def z_copy(i, source, target, columns):
        rows = pl.ds(pl.multiple_of(sent_at(i, top_pieces) * SPAN, SPAN), SPAN)
        return pltpu.make_async_remote_copy(
            src_ref=source.at[rows, columns],
            dst_ref=target.at[rows, columns],
            send_sem=zs.at[i],
            recv_sem=zr.at[i],
            device_id=(row, jnp.minimum(col + 1, cols_n - 1)),
            device_id_type=MESH,
        )

    def z_each(i, act):
        is_top = jnp.logical_and(row == 0, i < top_pieces)
        for k in range(groups):
            @pl.when(jnp.logical_and(is_top, i // per_block == k))
            def _(k=k):
                act(tile, top, upper(k))

        @pl.when(jnp.logical_not(is_top))
        def _():
            act(a_ref, zbuf, pl.ds(0, width))

    ahead = jnp.where(row == 0, AHEAD[0], AHEAD[1])

    def z_first(i):
        z_each(i, lambda source, target, columns: z_copy(i, source, target, columns).start())

    def z_step(i):
        @pl.when(panel)
        def _():
            z_each(i, lambda source, target, columns: z_copy(i, source, target, columns).wait_send())

            @pl.when(i + ahead < pieces)
            def _():
                z_first(i + ahead)

        @pl.when(col != 0)
        def _():
            def act(source, target, columns):
                z_copy(i, target, target, columns).wait_recv()

                @pl.when(relays)
                def _():
                    z_copy(i, target, target, columns).start()

            z_each(i, act)

    def z_sent(i):
        z_each(i, lambda source, target, columns: z_copy(i, target, target, columns).wait_send())

    def l_load(b):
        return pltpu.make_async_copy(
            l_ref.at[pl.ds(b * tile_n, tile_n)], out_ref.at[pl.ds(b * tile_n, tile_n)], here.at[b]
        )

    def base_load(b):
        return pltpu.make_async_copy(
            a_ref.at[pl.ds(b * tile_n, tile_n)], out_ref.at[pl.ds(b * tile_n, tile_n)], here.at[blocks + b]
        )

    def a_load(b):
        return pltpu.make_async_copy(
            a_ref.at[pl.ds(b * tile_n, tile_n)], zbuf.at[pl.ds(b * tile_n, tile_n)], here.at[2 * blocks + b]
        )

    extra = 3 * blocks
    inv_load = [
        pltpu.make_async_copy(
            i_ref.at[k], work.at[pl.ds(k * half, half), pl.ds(k * half, half)], here.at[extra + k]
        )
        for k in range(2)
    ]
    couple_load = pltpu.make_async_copy(l_ref.at[pl.ds(half, half), pl.ds(0, half)], couple, here.at[extra + 2])
    low_load = pltpu.make_async_copy(l_ref.at[pl.ds(offset, width)], low, here.at[extra + 3])
    top_load = pltpu.make_async_copy(a_ref.at[pl.ds(0, width)], top, here.at[extra + 4])
    is_root = jnp.logical_and(row == root, col != 0)
    first_top = jnp.logical_and(row == 0, panel)

    @pl.when(first_top)
    def _():
        top_load.start()

    for copy in inv_load:
        copy.start()

    @pl.loop(0, blocks)
    def _(b):
        l_load(b).start()

    barrier = pltpu.get_barrier_semaphore()
    for step in range(1, rows_n):
        pl.semaphore_signal(barrier, inc=1, device_id=((row + step) % rows_n, col), device_id_type=MESH)

    @pl.when(col != cols_n - 1)
    def _():
        pl.semaphore_signal(
            barrier, inc=1, device_id=(row, jnp.minimum(col + 1, cols_n - 1)), device_id_type=MESH
        )

    @pl.when(col != 0)
    def _():
        pl.semaphore_signal(barrier, inc=1, device_id=(row, jnp.maximum(col - 1, 0)), device_id_type=MESH)

    ends = jnp.where(col == 0, 1, 0) + jnp.where(col == cols_n - 1, 1, 0)
    pl.semaphore_wait(barrier, rows_n + 1 - ends)

    @pl.when(first_top)
    def _():
        top_load.wait()
        for k in range(groups):
            rows = slice(k * tile_n, (k + 1) * tile_n)
            for n in range(k, groups):
                columns = slice(n * tile_n, (n + 1) * tile_n)
                tile[rows, columns] = top[rows, columns] + top[columns, rows].T

    if cols_n > 1:
        @pl.when(panel)
        def _():
            @pl.loop(0, jnp.minimum(ahead, pieces))
            def _(i):
                z_first(i)

    @pl.when(row == 0)
    def _():
        couple_load.start()

    @pl.when(is_root)
    def _():
        low_load.start()

    @pl.when(panel)
    def _():
        @pl.loop(0, blocks)
        def _(b):
            a_load(b).start()

    def minus_eye(at, count):
        rows = lax.broadcasted_iota(jnp.int32, (count, width), 0) + at
        columns = lax.broadcasted_iota(jnp.int32, (count, width), 1)
        return jnp.where(rows == columns, -1.0, 0.0)

    strip = min(64, tile_n)
    strips = depth // strip

    def l_piece(i):
        per = tile_n // strip
        b = i // per
        rows = pl.ds(pl.multiple_of(i * strip, strip), strip)
        block = pl.ds(pl.multiple_of(b * tile_n, tile_n), tile_n)

        @pl.when(i % per == 0)
        def _():
            l_load(b).wait()

        is_top = jnp.logical_and(row == 0, i * strip < width)

        @pl.when(is_top)
        def _():
            lh[rows] = jnp.where(panel, minus_eye(i * strip, strip), 0.0).astype(jnp.bfloat16)
            ll[rows] = jnp.zeros((strip, width), jnp.bfloat16)

        @pl.when(jnp.logical_not(is_top))
        def _():
            lh[rows], ll[rows] = split(out_ref[rows])

        @pl.when(i % per == per - 1)
        def _():
            @pl.when(panel)
            def _():
                out_ref[block] = jnp.zeros((tile_n, width), f32)

            @pl.when(jnp.logical_not(panel))
            def _():
                base_load(b).start()

    def corner_piece(k):
        count = half // small

        @pl.when(k == 0)
        def _():
            for copy in inv_load:
                copy.wait()

            @pl.when(row == 0)
            def _():
                couple_load.wait()

            work[0:half, half:] = jnp.zeros((half, width - half), f32)

        rows = pl.ds(pl.multiple_of((k % count) * small, small), small)
        lower_rows = pl.ds(pl.multiple_of(half + (k % count) * small, small), small)

        @pl.when(k < count)
        def _():
            part[rows] = full_dot(couple[rows], work[0:half, 0:half])

        @pl.when(k >= count)
        def _():
            work[lower_rows, 0:half] = -full_dot(work[lower_rows, half:], part[...])

    def rows_of(b):
        return pl.ds(pl.multiple_of(b * tile_n, tile_n), tile_n)

    def inv_piece(b):
        ih[rows_of(b)], il[rows_of(b)] = split(work[rows_of(b)])

    def key_piece(b):
        @pl.when(b == 0)
        def _():
            @pl.when(is_root)
            def _():
                low_load.wait()

            @pl.loop(0, blocks)
            def _(k):
                @pl.when(jnp.logical_not(panel))
                def _():
                    base_load(k).wait()

                @pl.when(panel)
                def _():
                    a_load(k).wait()

        @pl.when(panel)
        def _():
            low[rows_of(b)] = minus_eye(b * tile_n, tile_n)

        for n in range(groups):
            at = n * tile_n
            columns = slice(at, at + tile_n)
            high, rest = split(low[rows_of(b), at:])
            kh[rows_of(b), columns], kl[rows_of(b), columns] = split(
                dot3(high, rest, ih[at:, columns], il[at:, columns], NN)
            )

    def row_piece(h):
        b, side = sent_at(h // 2, groups), h % 2

        @pl.when(jnp.logical_not(jnp.logical_and(row == 0, b * tile_n < width)))
        def _():
            columns = pl.ds(pl.multiple_of(side * (width // 2), width // 2), width // 2)
            high, rest = split(zbuf[rows_of(b)])
            out_ref[rows_of(b), columns] -= dot3(high, rest, kh[columns], kl[columns], NT)

    def top_piece(b):
        ch[rows_of(b)], cl[rows_of(b)] = split(top[rows_of(b)])

    def product_piece(h):
        b, group = h % groups, h // groups
        high, rest = kh.at[rows_of(b)], kl.at[rows_of(b)]
        for n in range(groups):
            own, at = slice(n * tile_n, (n + 1) * tile_n), (n + 1) * tile_n

            @pl.when(jnp.logical_and(group == n, panel))
            def _():
                work[rows_of(b), own] = dot3(high[...], rest[...], ch[own], cl[own], NT)

            @pl.when(jnp.logical_and(group == n, jnp.logical_not(panel)))
            def _():
                total = dot3(high[:, :at], rest[:, :at], ch[:at, own], cl[:at, own], NN)
                if n + 1 < groups:
                    total += dot3(high[:, at:], rest[:, at:], ch[own, at:], cl[own, at:], NT)
                work[rows_of(b), own] = 0.5 * total

    def weight_piece(j):
        own = pl.ds(pl.multiple_of((offset + j * tile_n) % depth, tile_n), tile_n)
        for mine, source, rows in ((row == root, zbuf, own), (row != root, tile, rows_of(j))):
            @pl.when(mine)
            def _(source=source, rows=rows):
                vh[...], vl[...] = split(jnp.where(panel, 0.0, source[rows]) - work[rows_of(j)])

        for n in reversed(range(groups)):
            at, end = n * tile_n, (n + 1) * tile_n
            vh[:, at:end], vl[:, at:end] = split(
                dot3(vh[:, :end], vl[:, :end], ih[at:end, :end], il[at:end, :end], NT)
            )

    big = min(2 * tile_n, depth)

    def column_piece(j, k):
        rows = pl.ds(pl.multiple_of(k * big, big), big)
        columns = pl.ds(pl.multiple_of(j * tile_n, tile_n), tile_n)
        out_ref[rows, columns] -= dot3(lh[rows], ll[rows], vh[...], vl[...], NT)

    corner_at = PACE * parts + most(COUPLE) * LAGS[COUPLE] + WAITS[COUPLE]
    corner_n = 2 * (half // small)
    inv_at = corner_at + corner_n
    key_at = max(inv_at + groups, LATER[LOWER] + PACE * (width // low_rows) + most(LOWER) * LAGS[LOWER] + WAITS[LOWER], strips)
    row_at = key_at + groups
    caught = 0
    while caught < blocks and per_block * (caught + 1) <= row_at + 2 * caught:
        caught += 1
    top_from = PACE - 1 + most(TOP) * LAGS[TOP] + WAITS[TOP]
    early_at = max(row_at + 2 * caught, top_from + per_block * (groups - 1))
    early_n = groups * (groups - 1)
    top_at = max(early_at + groups - 1 + early_n, top_from + top_pieces)
    weight_from = top_at + 1 + groups
    column_n = depth // big
    tile_from = tile_start + PACE - 1 + jnp.maximum(0, most(TILEROWS) * LAGS[TILEROWS] + wait(TILEROWS))
    last_tile = PACE - 1 + max((depth - width) // SPAN, LATER[TILEROWS]) + most(TILEROWS) * LAGS[TILEROWS] + max(WAITS[TILEROWS], 0)
    window = 1 + column_n
    apart = max(window, (pieces - weight_from - window) // groups)
    weight_starts = [
        jnp.maximum(weight_from + apart * j, tile_from + per_block * (j + 1)) for j in range(groups)
    ]
    steps = max(
        pieces + 2,
        max(weight_from + apart * (groups - 1), last_tile + per_block * groups) + window,
        top_at + groups,
    )

    def between(i, start, count):
        return jnp.logical_and(i >= start, i < start + count)

    @pl.loop(0, steps)
    def _(i):
        if cols_n > 1:
            @pl.when(i < pieces)
            def _():
                z_step(i)

            @pl.when(jnp.logical_and(relays, between(i, BEHIND, pieces)))
            def _():
                z_sent(i - BEHIND)

        if rows_n > 1:
            for item in range(4):
                p_step(item, i)

            @pl.when(i == top_at)
            def _():
                for item in (COUPLE, LOWER, TOP):
                    p_finish(item)

        for start, count, piece in (
            (0, strips, l_piece),
            (corner_at, corner_n, corner_piece),
            (inv_at, groups, inv_piece),
            (key_at, groups, key_piece),
        ):
            @pl.when(between(i, start, count))
            def _(start=start, piece=piece):
                piece(i - start)

        @pl.when(jnp.logical_or(between(i, early_at, groups - 1), i == top_at))
        def _():
            top_piece(jnp.where(i == top_at, groups - 1, i - early_at))

        @pl.when(jnp.logical_or(between(i, early_at + groups - 1, early_n), between(i, top_at + 1, groups)))
        def _():
            product_piece(jnp.where(i > top_at, early_n + i - top_at - 1, i - early_at - groups + 1))

        late = i // per_block - 1
        early = between(i, row_at, 2 * caught)
        in_time = jnp.logical_and(i % per_block < 2, jnp.logical_and(late >= caught, late < blocks))

        @pl.when(jnp.logical_or(early, in_time))
        def _():
            row_piece(jnp.where(early, i - row_at, 2 * late + i % per_block))

        group, at, busy = 0, 0, 0
        for j in range(groups):
            mine = between(i, weight_starts[j], window)
            group = group + jnp.where(mine, j, 0)
            at = at + jnp.where(mine, i - weight_starts[j], 0)
            busy = busy + jnp.where(mine, 1, 0)

        @pl.when(jnp.logical_and(busy > 0, at == 0))
        def _():
            weight_piece(group)

        @pl.when(jnp.logical_and(busy > 0, at > 0))
        def _():
            column_piece(group, at - 1)

    if cols_n > 1:
        @pl.when(relays)
        def _():
            @pl.loop(max(0, steps - BEHIND), pieces)
            def _(i):
                z_sent(i)

    if rows_n > 1:
        p_finish(TILEROWS)


def body(rows_n, cols_n, a_window, l_panel, l_inverse):
    depth, width = a_window.shape
    half = l_inverse.shape[1]
    f32, bf16 = jnp.float32, jnp.bfloat16
    tile_n = min(TILE, width)
    dma = pltpu.SemaphoreType.DMA
    pieces, top_pieces, low_pieces = depth // SPAN, width // (PACE * SPAN), width // (2 * PACE * SPAN)
    square = pltpu.VMEM((width, width), f32)
    narrow = pltpu.VMEM((width, width), bf16)
    return pl.pallas_call(
        functools.partial(step_kernel, rows_n, cols_n),
        out_shape=pltpu.VMEM((depth, width), f32),
        in_specs=[pl.BlockSpec(memory_space=pl.ANY)] * 3,
        out_specs=pl.BlockSpec(memory_space=pltpu.VMEM),
        scratch_shapes=[
            pltpu.VMEM((depth, width), f32),
            square,
            square,
            square,
            pltpu.VMEM((half, half), f32),
            pltpu.VMEM((half, half), f32),
            square,
            pltpu.VMEM((depth, width), bf16),
            pltpu.VMEM((depth, width), bf16),
            narrow,
            narrow,
            narrow,
            narrow,
            narrow,
            narrow,
            pltpu.VMEM((tile_n, width), bf16),
            pltpu.VMEM((tile_n, width), bf16),
            dma((pieces,)),
            dma((pieces,)),
            dma((2, couple_parts(half))),
            dma((couple_parts(half),)),
            dma((2, low_pieces)),
            dma((low_pieces,)),
            dma((2, top_pieces)),
            dma((top_pieces,)),
            dma((3, top_pieces)),
            dma((top_pieces,)),
            dma((3 * (depth // tile_n) + 5,)),
        ],
        compiler_params=pltpu.CompilerParams(
            collective_id=0, has_side_effects=True, vmem_limit_bytes=50 * 1024 * 1024
        ),
    )(a_window, l_panel, l_inverse)


def solution(mesh):
    placed = (P("row", "col"), P("row", None), P())
    return jax.shard_map(
        functools.partial(body, mesh.shape["row"], mesh.shape["col"]),
        mesh=mesh,
        in_specs=placed,
        out_specs=P("row", "col"),
        check_vma=False,
    )
```

```python
import functools

import jax
import jax.numpy as jnp
from jax import lax
from jax.experimental import pallas as pl
from jax.experimental.pallas import tpu as pltpu
from jax.sharding import PartitionSpec as P

MESH = pl.DeviceIdType.MESH
SPAN = 16
PACE = 2
TILE = 256
RECENT = 8
BEHIND = 12
AHEAD = (3, 24)
LAGS = (4, 4, 4, 3)
LATER = (0, 4, 0, 36)
WAITS = (6, 6, 6, -10, -4)
NN, NT = ((1,), (0,)), ((1,), (1,))
COUPLE, LOWER, TOP, TILEROWS = range(4)


def bits_of(count):
    return max(count.bit_length() - 1, 0)


def ring_pos(index, count):
    if count & (count - 1):
        return index
    parity, place = 0, 0
    for bit in reversed(range(bits_of(count))):
        parity = (parity + (index // 2**bit) % 2) % 2
        place = place + parity * 2**bit
    return place


def ring_at(place, count):
    if count & (count - 1):
        return place
    index = 0
    for bit in range(bits_of(count)):
        index = index + (((place // 2**bit) % 2 + (place // 2 ** (bit + 1)) % 2) % 2) * 2**bit
    return index


def seen_from(index, root, count):
    if count & (count - 1):
        return (index - root + count) % count
    return sum((((index // 2**bit) % 2 + (root // 2**bit) % 2) % 2) * 2**bit for bit in range(bits_of(count)))


def placed_from(offset, root, count):
    if count & (count - 1):
        return (offset + root) % count
    return seen_from(offset, root, count)


def couple_parts(half):
    return max(half // (2 * PACE * SPAN), 2)


def split(value):
    high = value.astype(jnp.bfloat16)
    return high, (value - high.astype(jnp.float32)).astype(jnp.bfloat16)


def dot3(left_high, left_low, high, low, dims):
    total = lax.dot_general(left_high, high, (dims, ((), ())), preferred_element_type=jnp.float32)
    total += lax.dot_general(left_high, low, (dims, ((), ())), preferred_element_type=jnp.float32)
    return total + lax.dot_general(left_low, high, (dims, ((), ())), preferred_element_type=jnp.float32)


def full_dot(left, right):
    return lax.dot_general(
        left, right, (NN, ((), ())), precision=lax.Precision.HIGHEST, preferred_element_type=jnp.float32
    )


def step_kernel(
    rows_n, cols_n, a_ref, l_ref, i_ref, out_ref,
    zbuf, top, tile, low, couple, part, work, lh, ll, ih, il, kh, kl, ch, cl, vh, vl,
    zs, zr, cs, cr, ls, lr, ts, tr, gs, gr, here,
):
    row, col = lax.axis_index("row"), lax.axis_index("col")
    depth, width = a_ref.shape
    half = i_ref.shape[1]
    pieces = depth // SPAN
    top_pieces = width // SPAN
    tile_n = min(TILE, width)
    blocks, groups = depth // tile_n, width // tile_n
    per_block = tile_n // SPAN
    small = min(128, half)
    panel = col == 0
    relays = jnp.logical_and(col != 0, col != cols_n - 1)
    root = (col * width) // depth
    offset = (col * width) % depth
    pair = 2 if rows_n % 2 == 0 else 1
    chain = rows_n // pair
    f32 = jnp.float32

    low_rows, own_rows = 2 * PACE * SPAN, PACE * SPAN
    parts = couple_parts(half)
    natural = row == 0
    turned = depth // width - 1 - offset // width
    tile_at = jnp.where(root == 0, offset // width, turned) * top_pieces
    tile_start = jnp.where(tile_at > 0, tile_at, LATER[TILEROWS])

    def sent_at(index, per):
        return jnp.where(natural, index, (depth // width - 1 - index // per) * per + index % per)

    items = (
        (couple, cs, cr, half // parts, parts, 0, 0),
        (low, ls, lr, low_rows, width // low_rows, root, LATER[LOWER]),
        (top, ts, tr, own_rows, width // own_rows, 0, PACE - 1),
        (tile, gs, gr, own_rows, width // own_rows, root, tile_start + PACE - 1),
    )

    rel, far, is_last, level, p_next, p_twin = [], [], [], [], [], []
    for item in range(4):
        origin = items[item][5]
        seen = seen_from(row, origin, rows_n)
        at = ring_pos(seen // pair, chain)
        odd = seen % pair
        ways = (at, (chain - at) % chain)
        short = item == TILEROWS and chain > 2
        rel.append(seen)
        far.append(ways)
        is_last.append(tuple(way >= chain - (2 if short else 1) for way in ways))
        if item == TILEROWS:
            ways = tuple(jnp.where(way == chain - 1, jnp.minimum(way, 1), way) for way in ways)
        level.append(tuple(way + odd for way in ways))
        p_next.append(
            tuple(
                placed_from(ring_at((at + (1 if way == 0 else chain - 1)) % chain, chain) * pair, origin, rows_n)
                for way in range(2)
            )
        )
        p_twin.append(placed_from(seen + (pair - 1) * (1 - odd), origin, rows_n))

    def wait(item):
        if item != TILEROWS:
            return WAITS[item]
        return jnp.where(tile_at > 0, jnp.where(root == 0, WAITS[item], WAITS[item + 1]), 0)

    begins = [
        tuple(items[item][6] + jnp.where(of_way > 0, of_way * LAGS[item] + wait(item), 0) for of_way in level[item])
        for item in range(4)
    ]
    sends_on = [rel[item] % pair == 0 for item in range(4)]
    is_first = [rel[item] == 0 for item in range(4)]

    def most(item):
        chips = max(chain - 2, 1) if item == TILEROWS and chain > 1 else chain - 1
        return chips + pair - 1

    def p_copy(item, kind, at, source, first, columns, target):
        buffer, send, recv, count = items[item][:4]
        return pltpu.make_async_remote_copy(
            src_ref=source.at[pl.ds(first + at * count, count), columns],
            dst_ref=buffer.at[pl.ds(at * count, count), columns],
            send_sem=send.at[kind, at],
            recv_sem=recv.at[at],
            device_id=(target, col),
            device_id_type=MESH,
        )

    def upper(k):
        return pl.ds(k * tile_n, width - k * tile_n)

    def each(item, at, act):
        if item != TOP:
            act(pl.ds(0, items[item][0].shape[1]))
            return

        @pl.when(panel)
        def _():
            act(pl.ds(0, width))

        for k in range(groups):
            @pl.when(jnp.logical_and(jnp.logical_not(panel), at // (tile_n // own_rows) == k))
            def _(k=k):
                act(upper(k))

    def p_send(item, way, at, source, first, columns):
        if chain > 1:
            @pl.when(jnp.logical_not(is_last[item][way]))
            def _():
                p_copy(item, 0, at, source, first, columns, p_next[item][way]).start()

        if chain > 2 and item == TILEROWS:
            @pl.when(is_first[item])
            def _():
                p_copy(item, 2, at, source, first, columns, p_next[item][1 - way]).start()

        if pair > 1:
            p_copy(item, 1, at, source, first, columns, p_twin[item]).start()

    def p_first(item, way, at, columns):
        if item == COUPLE:
            p_send(item, way, at, l_ref, half, columns)
        elif item == LOWER:
            p_send(item, way, at, l_ref, offset, columns)
        elif item == TOP:
            @pl.when(panel)
            def _():
                p_send(item, way, at, a_ref, 0, columns)

            @pl.when(jnp.logical_not(panel))
            def _():
                p_send(item, way, at, top, 0, columns)
        else:
            p_send(item, way, at, zbuf, offset, columns)

    wanted = [col != 0 if item in (LOWER, TILEROWS) else col >= 0 for item in range(4)]

    def p_step(item, i):
        count = items[item][4]
        for way in range(2):
            since = i - begins[item][way]
            at = since // PACE

            @pl.when(
                jnp.logical_and(wanted[item], jnp.logical_and(jnp.logical_and(since >= 0, at < count), since % (2 * PACE) == way * PACE))
            )
            def _():
                def act(columns):
                    @pl.when(is_first[item])
                    def _():
                        p_first(item, way, at, columns)

                    @pl.when(jnp.logical_not(is_first[item]))
                    def _():
                        buffer = items[item][0]
                        p_copy(item, 0, at, buffer, 0, columns, row).wait_recv()

                        @pl.when(sends_on[item])
                        def _():
                            p_send(item, way, at, buffer, 0, columns)

                each(item, at, act)

                if item == TILEROWS:
                    @pl.when(jnp.logical_and(sends_on[item], at >= RECENT))
                    def _():
                        p_sent(item, at - RECENT)

    def p_sent(item, at):
        buffer = items[item][0]

        def act(columns):
            for way in range(2):
                if chain > 1:
                    @pl.when(jnp.logical_and(at % 2 == way, jnp.logical_not(is_last[item][way])))
                    def _():
                        p_copy(item, 0, at, buffer, 0, columns, row).wait_send()

            if chain > 2 and item == TILEROWS:
                @pl.when(is_first[item])
                def _():
                    p_copy(item, 2, at, buffer, 0, columns, row).wait_send()

            if pair > 1:
                p_copy(item, 1, at, buffer, 0, columns, row).wait_send()

        each(item, at, act)

    def p_finish(item):
        held = RECENT if item == TILEROWS else items[item][4]

        @pl.when(jnp.logical_and(wanted[item], sends_on[item]))
        def _():
            @pl.loop(max(0, items[item][4] - held), items[item][4])
            def _(at):
                p_sent(item, at)

    def z_copy(i, source, target, columns):
        rows = pl.ds(pl.multiple_of(sent_at(i, top_pieces) * SPAN, SPAN), SPAN)
        return pltpu.make_async_remote_copy(
            src_ref=source.at[rows, columns],
            dst_ref=target.at[rows, columns],
            send_sem=zs.at[i],
            recv_sem=zr.at[i],
            device_id=(row, jnp.minimum(col + 1, cols_n - 1)),
            device_id_type=MESH,
        )

    def z_each(i, act):
        is_top = jnp.logical_and(row == 0, i < top_pieces)
        for k in range(groups):
            @pl.when(jnp.logical_and(is_top, i // per_block == k))
            def _(k=k):
                act(tile, top, upper(k))

        @pl.when(jnp.logical_not(is_top))
        def _():
            act(a_ref, zbuf, pl.ds(0, width))

    ahead = jnp.where(row == 0, AHEAD[0], AHEAD[1])

    def z_first(i):
        z_each(i, lambda source, target, columns: z_copy(i, source, target, columns).start())

    def z_step(i):
        @pl.when(panel)
        def _():
            z_each(i, lambda source, target, columns: z_copy(i, source, target, columns).wait_send())

            @pl.when(i + ahead < pieces)
            def _():
                z_first(i + ahead)

        @pl.when(col != 0)
        def _():
            def act(source, target, columns):
                z_copy(i, target, target, columns).wait_recv()

                @pl.when(relays)
                def _():
                    z_copy(i, target, target, columns).start()

            z_each(i, act)

    def z_sent(i):
        z_each(i, lambda source, target, columns: z_copy(i, target, target, columns).wait_send())

    def l_load(b):
        return pltpu.make_async_copy(
            l_ref.at[pl.ds(b * tile_n, tile_n)], out_ref.at[pl.ds(b * tile_n, tile_n)], here.at[b]
        )

    def base_load(b):
        return pltpu.make_async_copy(
            a_ref.at[pl.ds(b * tile_n, tile_n)], out_ref.at[pl.ds(b * tile_n, tile_n)], here.at[blocks + b]
        )

    def a_load(b):
        return pltpu.make_async_copy(
            a_ref.at[pl.ds(b * tile_n, tile_n)], zbuf.at[pl.ds(b * tile_n, tile_n)], here.at[2 * blocks + b]
        )

    extra = 3 * blocks
    inv_load = [
        pltpu.make_async_copy(
            i_ref.at[k], work.at[pl.ds(k * half, half), pl.ds(k * half, half)], here.at[extra + k]
        )
        for k in range(2)
    ]
    couple_load = pltpu.make_async_copy(l_ref.at[pl.ds(half, half), pl.ds(0, half)], couple, here.at[extra + 2])
    low_load = pltpu.make_async_copy(l_ref.at[pl.ds(offset, width)], low, here.at[extra + 3])
    top_load = pltpu.make_async_copy(a_ref.at[pl.ds(0, width)], top, here.at[extra + 4])
    is_root = jnp.logical_and(row == root, col != 0)
    first_top = jnp.logical_and(row == 0, panel)

    @pl.when(first_top)
    def _():
        top_load.start()

    for copy in inv_load:
        copy.start()

    @pl.loop(0, blocks)
    def _(b):
        l_load(b).start()

    barrier = pltpu.get_barrier_semaphore()
    for step in range(1, rows_n):
        pl.semaphore_signal(barrier, inc=1, device_id=((row + step) % rows_n, col), device_id_type=MESH)

    @pl.when(col != cols_n - 1)
    def _():
        pl.semaphore_signal(
            barrier, inc=1, device_id=(row, jnp.minimum(col + 1, cols_n - 1)), device_id_type=MESH
        )

    @pl.when(col != 0)
    def _():
        pl.semaphore_signal(barrier, inc=1, device_id=(row, jnp.maximum(col - 1, 0)), device_id_type=MESH)

    ends = jnp.where(col == 0, 1, 0) + jnp.where(col == cols_n - 1, 1, 0)
    pl.semaphore_wait(barrier, rows_n + 1 - ends)

    @pl.when(first_top)
    def _():
        top_load.wait()
        for k in range(groups):
            rows = slice(k * tile_n, (k + 1) * tile_n)
            for n in range(k, groups):
                columns = slice(n * tile_n, (n + 1) * tile_n)
                tile[rows, columns] = top[rows, columns] + top[columns, rows].T

    if cols_n > 1:
        @pl.when(panel)
        def _():
            @pl.loop(0, jnp.minimum(ahead, pieces))
            def _(i):
                z_first(i)

    @pl.when(row == 0)
    def _():
        couple_load.start()

    @pl.when(is_root)
    def _():
        low_load.start()

    @pl.when(panel)
    def _():
        @pl.loop(0, blocks)
        def _(b):
            a_load(b).start()

    def minus_eye(at, count):
        rows = lax.broadcasted_iota(jnp.int32, (count, width), 0) + at
        columns = lax.broadcasted_iota(jnp.int32, (count, width), 1)
        return jnp.where(rows == columns, -1.0, 0.0)

    strip = min(64, tile_n)
    strips = depth // strip

    def l_piece(i):
        per = tile_n // strip
        b = i // per
        rows = pl.ds(pl.multiple_of(i * strip, strip), strip)
        block = pl.ds(pl.multiple_of(b * tile_n, tile_n), tile_n)

        @pl.when(i % per == 0)
        def _():
            l_load(b).wait()

        is_top = jnp.logical_and(row == 0, i * strip < width)

        @pl.when(is_top)
        def _():
            lh[rows] = jnp.where(panel, minus_eye(i * strip, strip), 0.0).astype(jnp.bfloat16)
            ll[rows] = jnp.zeros((strip, width), jnp.bfloat16)

        @pl.when(jnp.logical_not(is_top))
        def _():
            lh[rows], ll[rows] = split(out_ref[rows])

        @pl.when(i % per == per - 1)
        def _():
            @pl.when(panel)
            def _():
                out_ref[block] = jnp.zeros((tile_n, width), f32)

            @pl.when(jnp.logical_not(panel))
            def _():
                base_load(b).start()

    def corner_piece(k):
        count = half // small

        @pl.when(k == 0)
        def _():
            for copy in inv_load:
                copy.wait()

            @pl.when(row == 0)
            def _():
                couple_load.wait()

            work[0:half, half:] = jnp.zeros((half, width - half), f32)

        rows = pl.ds(pl.multiple_of((k % count) * small, small), small)
        lower_rows = pl.ds(pl.multiple_of(half + (k % count) * small, small), small)

        @pl.when(k < count)
        def _():
            part[rows] = full_dot(couple[rows], work[0:half, 0:half])

        @pl.when(k >= count)
        def _():
            work[lower_rows, 0:half] = -full_dot(work[lower_rows, half:], part[...])

    def rows_of(b):
        return pl.ds(pl.multiple_of(b * tile_n, tile_n), tile_n)

    def inv_piece(b):
        ih[rows_of(b)], il[rows_of(b)] = split(work[rows_of(b)])

    def key_piece(b):
        @pl.when(b == 0)
        def _():
            @pl.when(is_root)
            def _():
                low_load.wait()

            @pl.loop(0, blocks)
            def _(k):
                @pl.when(jnp.logical_not(panel))
                def _():
                    base_load(k).wait()

                @pl.when(panel)
                def _():
                    a_load(k).wait()

        @pl.when(panel)
        def _():
            low[rows_of(b)] = minus_eye(b * tile_n, tile_n)

        for n in range(groups):
            at = n * tile_n
            columns = slice(at, at + tile_n)
            high, rest = split(low[rows_of(b), at:])
            kh[rows_of(b), columns], kl[rows_of(b), columns] = split(
                dot3(high, rest, ih[at:, columns], il[at:, columns], NN)
            )

    def row_piece(h):
        b, side = sent_at(h // 2, groups), h % 2

        @pl.when(jnp.logical_not(jnp.logical_and(row == 0, b * tile_n < width)))
        def _():
            columns = pl.ds(pl.multiple_of(side * (width // 2), width // 2), width // 2)
            high, rest = split(zbuf[rows_of(b)])
            out_ref[rows_of(b), columns] -= dot3(high, rest, kh[columns], kl[columns], NT)

    fine = tile_n // 2

    def last_piece(part, side):
        first = sent_at(blocks - 1, groups) * tile_n + part * fine

        @pl.when(jnp.logical_not(jnp.logical_and(row == 0, first < width)))
        def _():
            rows = pl.ds(pl.multiple_of(first, fine), fine)
            columns = pl.ds(pl.multiple_of(side * (width // 2), width // 2), width // 2)
            high, rest = split(zbuf[rows])
            out_ref[rows, columns] -= dot3(high, rest, kh[columns], kl[columns], NT)

    def top_piece(b):
        ch[rows_of(b)], cl[rows_of(b)] = split(top[rows_of(b)])

    def product_piece(h):
        b, group = h % groups, h // groups
        high, rest = kh.at[rows_of(b)], kl.at[rows_of(b)]
        for n in range(groups):
            own, at = slice(n * tile_n, (n + 1) * tile_n), (n + 1) * tile_n

            @pl.when(jnp.logical_and(group == n, panel))
            def _():
                work[rows_of(b), own] = dot3(high[...], rest[...], ch[own], cl[own], NT)

            @pl.when(jnp.logical_and(group == n, jnp.logical_not(panel)))
            def _():
                total = dot3(high[:, :at], rest[:, :at], ch[:at, own], cl[:at, own], NN)
                if n + 1 < groups:
                    total += dot3(high[:, at:], rest[:, at:], ch[own, at:], cl[own, at:], NT)
                work[rows_of(b), own] = 0.5 * total

    def weight_piece(j):
        own = pl.ds(pl.multiple_of((offset + j * tile_n) % depth, tile_n), tile_n)
        for mine, source, rows in ((row == root, zbuf, own), (row != root, tile, rows_of(j))):
            @pl.when(mine)
            def _(source=source, rows=rows):
                vh[...], vl[...] = split(jnp.where(panel, 0.0, source[rows]) - work[rows_of(j)])

        for n in reversed(range(groups)):
            at, end = n * tile_n, (n + 1) * tile_n
            vh[:, at:end], vl[:, at:end] = split(
                dot3(vh[:, :end], vl[:, :end], ih[at:end, :end], il[at:end, :end], NT)
            )

    big = min(2 * tile_n, depth)

    def column_piece(j, k):
        rows = pl.ds(pl.multiple_of(k * big, big), big)
        columns = pl.ds(pl.multiple_of(j * tile_n, tile_n), tile_n)
        out_ref[rows, columns] -= dot3(lh[rows], ll[rows], vh[...], vl[...], NT)

    corner_at = PACE * parts + most(COUPLE) * LAGS[COUPLE] + WAITS[COUPLE]
    corner_n = 2 * (half // small)
    inv_at = corner_at + corner_n
    key_at = max(inv_at + groups, LATER[LOWER] + PACE * (width // low_rows) + most(LOWER) * LAGS[LOWER] + WAITS[LOWER], strips)
    row_at = key_at + groups
    caught = 0
    while caught < blocks and per_block * (caught + 1) <= row_at + 2 * caught:
        caught += 1
    top_from = PACE - 1 + most(TOP) * LAGS[TOP] + WAITS[TOP]
    early_at = max(row_at + 2 * caught, top_from + per_block * (groups - 1))
    early_n = groups * (groups - 1)
    top_at = max(early_at + groups - 1 + early_n, top_from + top_pieces)
    weight_from = top_at + 1 + groups
    column_n = depth // big
    tile_from = tile_start + PACE - 1 + jnp.maximum(0, most(TILEROWS) * LAGS[TILEROWS] + wait(TILEROWS))
    last_tile = PACE - 1 + max((depth - width) // SPAN, LATER[TILEROWS]) + most(TILEROWS) * LAGS[TILEROWS] + max(WAITS[TILEROWS], 0)
    window = 1 + column_n
    apart = max(window, (pieces - weight_from - window) // groups)
    weight_starts = [
        jnp.maximum(weight_from + apart * j, tile_from + per_block * (j + 1)) for j in range(groups)
    ]
    steps = max(
        pieces + 2,
        max(weight_from + apart * (groups - 1), last_tile + per_block * groups) + window,
        top_at + groups,
    )

    def between(i, start, count):
        return jnp.logical_and(i >= start, i < start + count)

    @pl.loop(0, steps)
    def _(i):
        if cols_n > 1:
            @pl.when(i < pieces)
            def _():
                z_step(i)

            @pl.when(jnp.logical_and(relays, between(i, BEHIND, pieces)))
            def _():
                z_sent(i - BEHIND)

        if rows_n > 1:
            for item in range(4):
                p_step(item, i)

            @pl.when(i == top_at)
            def _():
                for item in (COUPLE, LOWER, TOP):
                    p_finish(item)

        for start, count, piece in (
            (0, strips, l_piece),
            (corner_at, corner_n, corner_piece),
            (inv_at, groups, inv_piece),
            (key_at, groups, key_piece),
        ):
            @pl.when(between(i, start, count))
            def _(start=start, piece=piece):
                piece(i - start)

        @pl.when(jnp.logical_or(between(i, early_at, groups - 1), i == top_at))
        def _():
            top_piece(jnp.where(i == top_at, groups - 1, i - early_at))

        @pl.when(jnp.logical_or(between(i, early_at + groups - 1, early_n), between(i, top_at + 1, groups)))
        def _():
            product_piece(jnp.where(i > top_at, early_n + i - top_at - 1, i - early_at - groups + 1))

        late = i // per_block - 1
        early = between(i, row_at, 2 * caught)
        in_time = jnp.logical_and(i % per_block < 2, jnp.logical_and(late >= caught, late < blocks - 1))

        @pl.when(jnp.logical_or(early, in_time))
        def _():
            row_piece(jnp.where(early, i - row_at, 2 * late + i % per_block))

        if caught < blocks:
            at_first = between(i, pieces - per_block // 2, 2)

            @pl.when(jnp.logical_or(at_first, between(i, pieces, 2)))
            def _():
                last_piece(jnp.where(at_first, 0, 1), i % 2)

        group, at, busy = 0, 0, 0
        for j in range(groups):
            mine = between(i, weight_starts[j], window)
            group = group + jnp.where(mine, j, 0)
            at = at + jnp.where(mine, i - weight_starts[j], 0)
            busy = busy + jnp.where(mine, 1, 0)

        @pl.when(jnp.logical_and(busy > 0, at == 0))
        def _():
            weight_piece(group)

        @pl.when(jnp.logical_and(busy > 0, at > 0))
        def _():
            column_piece(group, at - 1)

    if cols_n > 1:
        @pl.when(relays)
        def _():
            @pl.loop(max(0, steps - BEHIND), pieces)
            def _(i):
                z_sent(i)

    if rows_n > 1:
        p_finish(TILEROWS)


def body(rows_n, cols_n, a_window, l_panel, l_inverse):
    depth, width = a_window.shape
    half = l_inverse.shape[1]
    f32, bf16 = jnp.float32, jnp.bfloat16
    tile_n = min(TILE, width)
    dma = pltpu.SemaphoreType.DMA
    pieces, top_pieces, low_pieces = depth // SPAN, width // (PACE * SPAN), width // (2 * PACE * SPAN)
    square = pltpu.VMEM((width, width), f32)
    narrow = pltpu.VMEM((width, width), bf16)
    return pl.pallas_call(
        functools.partial(step_kernel, rows_n, cols_n),
        out_shape=pltpu.VMEM((depth, width), f32),
        in_specs=[pl.BlockSpec(memory_space=pl.ANY)] * 3,
        out_specs=pl.BlockSpec(memory_space=pltpu.VMEM),
        scratch_shapes=[
            pltpu.VMEM((depth, width), f32),
            square,
            square,
            square,
            pltpu.VMEM((half, half), f32),
            pltpu.VMEM((half, half), f32),
            square,
            pltpu.VMEM((depth, width), bf16),
            pltpu.VMEM((depth, width), bf16),
            narrow,
            narrow,
            narrow,
            narrow,
            narrow,
            narrow,
            pltpu.VMEM((tile_n, width), bf16),
            pltpu.VMEM((tile_n, width), bf16),
            dma((pieces,)),
            dma((pieces,)),
            dma((2, couple_parts(half))),
            dma((couple_parts(half),)),
            dma((2, low_pieces)),
            dma((low_pieces,)),
            dma((2, top_pieces)),
            dma((top_pieces,)),
            dma((3, top_pieces)),
            dma((top_pieces,)),
            dma((3 * (depth // tile_n) + 5,)),
        ],
        compiler_params=pltpu.CompilerParams(
            collective_id=0, has_side_effects=True, vmem_limit_bytes=50 * 1024 * 1024
        ),
    )(a_window, l_panel, l_inverse)


def solution(mesh):
    placed = (P("row", "col"), P("row", None), P())
    return jax.shard_map(
        functools.partial(body, mesh.shape["row"], mesh.shape["col"]),
        mesh=mesh,
        in_specs=placed,
        out_specs=P("row", "col"),
        check_vma=False,
    )
```
